16 devices in a mesh: rep: 2 (over z), fsdp: 8 (over y, x, core).
Axes of the slice: x: 2, y: 2, z: 2, core: 2. Of those that a mesh axis runs over, the one named last changes fastest.
Arguments:
- x_tokens: bfloat16 [192, 197, 1024], P(('rep', 'fsdp'))
- grad_z: bfloat16 [192, 197, 1024], P(('rep', 'fsdp'))
- w_qkv: float32 [1024, 3072], P('fsdp')
- b_qkv: float32 [3072], P('fsdp')
- w_out: float32 [1024, 1024], P('fsdp')
- w_up: float32 [1024, 4096], P('fsdp')
- b_up: float32 [4096], P('fsdp')
- w_down: float32 [4096, 1024], P('fsdp')
- vec_params: float32 [8, 1024], P(None, 'fsdp')
Outputs:
- output 1: bfloat16 [192, 197, 1024], P(('rep', 'fsdp'))
- output 2: bfloat16 [192, 197, 1024], P(('rep', 'fsdp'))
- output 3: float32 [1024, 3072], P('fsdp')
- output 4: float32 [3072], P('fsdp')
- output 5: float32 [1024, 1024], P('fsdp')
- output 6: float32 [1024, 4096], P('fsdp')
- output 7: float32 [4096], P('fsdp')
- output 8: float32 [4096, 1024], P('fsdp')
- output 9: float32 [8, 1024], P(None, 'fsdp')
All inputs are finite; a program needn't handle non-finite values.
Results may differ from the reference program's by a relative error of at most 0.02.
Values are sent between devices in bfloat16 or wider.
A program may use at most 1 GiB of HBM per device.

```python
import jax
import jax.numpy as jnp
from jax import lax

D = 1024
FF = 4096
SEQ = 197
HEADS = 16
SEQS_DEV = 12
DEVICES = 16
BATCH = SEQS_DEV * DEVICES
HEAD = D // HEADS
LN_EPS = 1e-5


def setup_inputs(seed: int = 0) -> dict:
    keys = jax.random.split(jax.random.key(seed), 12)
    seq_scale = jax.random.uniform(keys[0], (BATCH, 1, 1), minval=0.5, maxval=2.0)
    x_tokens = (jax.random.normal(keys[1], (BATCH, SEQ, D)) * seq_scale).astype(jnp.bfloat16)
    grad_scale = jax.random.uniform(keys[2], (BATCH, 1, 1), minval=0.25, maxval=2.0)
    grad_z = (jax.random.normal(keys[3], (BATCH, SEQ, D)) * grad_scale).astype(jnp.bfloat16)
    w_qkv = jax.random.normal(keys[4], (D, 3 * D)) * D ** -0.5
    b_qkv = 0.5 * jax.random.normal(keys[5], (3 * D,))
    w_out = jax.random.normal(keys[6], (D, D)) * D ** -0.5
    w_up = jax.random.normal(keys[7], (D, FF)) * D ** -0.5
    b_up = 0.5 * jax.random.normal(keys[8], (FF,))
    w_down = jax.random.normal(keys[9], (FF, D)) * FF ** -0.5
    is_scale = jnp.array([0.0, 0.0, 0.0, 1.0, 0.0, 0.0, 0.0, 1.0], jnp.float32)[:, None]
    row_offset = jnp.array([1.0, 0.0, 0.0, 0.0, 1.0, 0.0, 0.0, 0.0], jnp.float32)[:, None]
    normal_rows = row_offset + 0.25 * jax.random.normal(keys[10], (8, D))
    scale_rows = jax.random.uniform(keys[11], (8, D), minval=0.5, maxval=1.5)
    vec_params = is_scale * scale_rows + (1.0 - is_scale) * normal_rows
    return {"x_tokens": x_tokens, "grad_z": grad_z, "w_qkv": w_qkv, "b_qkv": b_qkv, "w_out": w_out,
            "w_up": w_up, "b_up": b_up, "w_down": w_down, "vec_params": vec_params}


def normalize(t):
    mean = jnp.mean(t, axis=-1, keepdims=True)
    centered = t - mean
    variance = jnp.mean(centered * centered, axis=-1, keepdims=True)
    return centered * lax.rsqrt(variance + LN_EPS)


def gelu_exact(t):
    return jax.nn.gelu(t, approximate=False)


def layer_pass(x_seq, dz_seq, matrices, bias_qkv, bias_up, vec_rows):
    w_qkv, w_out, w_up, w_down = matrices
    ln1_gain, ln1_bias, out_bias, scale_attn, ln2_gain, ln2_bias, down_bias, scale_mlp = vec_rows
    score_scale = HEAD ** -0.5
    x_float = x_seq.astype(jnp.float32)
    xhat_one, norm_one_back = jax.vjp(normalize, x_float)
    h_one = (xhat_one * ln1_gain + ln1_bias).astype(jnp.bfloat16)
    qkv_proj = (jnp.dot(h_one, w_qkv, preferred_element_type=jnp.float32) + bias_qkv).astype(jnp.bfloat16)
    qkv_heads = qkv_proj.reshape(SEQ, 3, HEADS, HEAD).astype(jnp.float32)
    q_heads = qkv_heads[:, 0]
    k_heads = qkv_heads[:, 1]
    v_heads = qkv_heads[:, 2]
    scores = jnp.einsum("qhe,khe->hqk", q_heads, k_heads) * score_scale
    attn_probs = jax.nn.softmax(scores, axis=-1)
    probs_bf = attn_probs.astype(jnp.bfloat16).astype(jnp.float32)
    head_out = jnp.einsum("hqk,khe->qhe", probs_bf, v_heads).astype(jnp.bfloat16).reshape(SEQ, D)
    att_out = jnp.dot(head_out, w_out, preferred_element_type=jnp.float32) + out_bias
    resid_mid = x_float + scale_attn * att_out
    xhat_two, norm_two_back = jax.vjp(normalize, resid_mid)
    h_two = (xhat_two * ln2_gain + ln2_bias).astype(jnp.bfloat16)
    pre_act = jnp.dot(h_two, w_up, preferred_element_type=jnp.float32) + bias_up
    act_float, gelu_back = jax.vjp(gelu_exact, pre_act)
    mlp_act = act_float.astype(jnp.bfloat16)
    mlp_out = jnp.dot(mlp_act, w_down, preferred_element_type=jnp.float32) + down_bias
    z_seq = (resid_mid + scale_mlp * mlp_out).astype(jnp.bfloat16)
    g_out = dz_seq.astype(jnp.float32)
    grad_scale_mlp = jnp.sum(g_out * mlp_out, axis=0)
    d_mlp = g_out * scale_mlp
    grad_down_bias = jnp.sum(d_mlp, axis=0)
    d_mlp_bf = d_mlp.astype(jnp.bfloat16)
    grad_w_down = jnp.dot(mlp_act.T, d_mlp_bf, preferred_element_type=jnp.float32)
    d_act = jnp.dot(d_mlp_bf, w_down.T, preferred_element_type=jnp.float32)
    d_pre = gelu_back(d_act)[0]
    grad_b_up = jnp.sum(d_pre, axis=0)
    d_pre_bf = d_pre.astype(jnp.bfloat16)
    grad_w_up = jnp.dot(h_two.T, d_pre_bf, preferred_element_type=jnp.float32)
    d_h_two = jnp.dot(d_pre_bf, w_up.T, preferred_element_type=jnp.float32)
    grad_ln2_gain = jnp.sum(d_h_two * xhat_two, axis=0)
    grad_ln2_bias = jnp.sum(d_h_two, axis=0)
    g_resid = g_out + norm_two_back(d_h_two * ln2_gain)[0]
    grad_scale_attn = jnp.sum(g_resid * att_out, axis=0)
    d_att = g_resid * scale_attn
    grad_out_bias = jnp.sum(d_att, axis=0)
    d_att_bf = d_att.astype(jnp.bfloat16)
    grad_w_out = jnp.dot(head_out.T, d_att_bf, preferred_element_type=jnp.float32)
    d_heads = jnp.dot(d_att_bf, w_out.T, preferred_element_type=jnp.float32).astype(jnp.bfloat16)
    d_heads = d_heads.reshape(SEQ, HEADS, HEAD).astype(jnp.float32)
    d_probs = jnp.einsum("qhe,khe->hqk", d_heads, v_heads)
    grad_v = jnp.einsum("hqk,qhe->khe", probs_bf, d_heads)
    d_scores = attn_probs * (d_probs - jnp.sum(d_probs * attn_probs, axis=-1, keepdims=True))
    d_scores_bf = (d_scores * score_scale).astype(jnp.bfloat16).astype(jnp.float32)
    grad_q = jnp.einsum("hqk,khe->qhe", d_scores_bf, k_heads)
    grad_k = jnp.einsum("hqk,qhe->khe", d_scores_bf, q_heads)
    d_qkv = jnp.stack([grad_q, grad_k, grad_v], axis=1).reshape(SEQ, 3 * D)
    grad_b_qkv = jnp.sum(d_qkv, axis=0)
    d_qkv_bf = d_qkv.astype(jnp.bfloat16)
    grad_w_qkv = jnp.dot(h_one.T, d_qkv_bf, preferred_element_type=jnp.float32)
    d_h_one = jnp.dot(d_qkv_bf, w_qkv.T, preferred_element_type=jnp.float32)
    grad_ln1_gain = jnp.sum(d_h_one * xhat_one, axis=0)
    grad_ln1_bias = jnp.sum(d_h_one, axis=0)
    dx_seq = (g_resid + norm_one_back(d_h_one * ln1_gain)[0]).astype(jnp.bfloat16)
    grad_vec = jnp.stack([grad_ln1_gain, grad_ln1_bias, grad_out_bias, grad_scale_attn,
                          grad_ln2_gain, grad_ln2_bias, grad_down_bias, grad_scale_mlp])
    return z_seq, dx_seq, (grad_w_qkv, grad_b_qkv, grad_w_out, grad_w_up, grad_b_up, grad_w_down, grad_vec)


def reference(x_tokens, grad_z, w_qkv, b_qkv, w_out, w_up, b_up, w_down, vec_params):
    matrices = (w_qkv.astype(jnp.bfloat16), w_out.astype(jnp.bfloat16),
                w_up.astype(jnp.bfloat16), w_down.astype(jnp.bfloat16))
    bias_qkv = b_qkv.astype(jnp.bfloat16).astype(jnp.float32)
    bias_up = b_up.astype(jnp.bfloat16).astype(jnp.float32)
    vec_rows = vec_params.astype(jnp.bfloat16).astype(jnp.float32)

    def step(running, pair):
        z_seq, dx_seq, seq_grads = layer_pass(pair[0], pair[1], matrices, bias_qkv, bias_up, vec_rows)
        return jax.tree.map(jnp.add, running, seq_grads), (z_seq, dx_seq)

    zero_grads = (jnp.zeros((D, 3 * D), jnp.float32), jnp.zeros((3 * D,), jnp.float32),
                  jnp.zeros((D, D), jnp.float32), jnp.zeros((D, FF), jnp.float32),
                  jnp.zeros((FF,), jnp.float32), jnp.zeros((FF, D), jnp.float32),
                  jnp.zeros((8, D), jnp.float32))
    totals, seq_outs = lax.scan(step, zero_grads, (x_tokens, grad_z))
    grad_w_qkv, grad_b_qkv, grad_w_out, grad_w_up, grad_b_up, grad_w_down, grad_vec = totals
    return (seq_outs[0], seq_outs[1], grad_w_qkv, grad_b_qkv, grad_w_out, grad_w_up, grad_b_up,
            grad_w_down, grad_vec)
```

```python
import functools

import jax
import jax.numpy as jnp
from jax import lax
from jax.experimental import pallas as pl
from jax.experimental.pallas import tpu as pltpu
from jax.sharding import PartitionSpec as P

HEADS = 16
LN_EPS = 1e-5
PAD = 200


def swap(value, mask):
    if mask == 8:
        return lax.ppermute(value, "rep", [(0, 1), (1, 0)])
    return lax.ppermute(value, "fsdp", [(i, i ^ mask) for i in range(8)])


def pick(value, index, axis):
    return lax.dynamic_index_in_dim(value, index, axis, keepdims=False)


def grad_send_kernel(order_ref, *refs):
    *a_refs, b_ref, out_ref = refs
    for j, a_ref in enumerate(a_refs):
        out_ref[j] = dot(a_ref[...], b_ref[...], ((0,), (0,)))


def grad_keep_kernel(order_ref, *refs, wide):
    *a_refs, b_ref, got_ref, keep_x, send_x, keep_y, send_y = refs
    step = pl.program_id(0)

    def write(ref, at, value):
        ref[at] = value

    for j, a_ref in enumerate(a_refs):
        total = dot(a_ref[...], b_ref[...], ((0,), (0,))) + got_ref[j]
        if wide:
            cut = total.shape[1] // 2
            along_y, along_x = step // 2, step % 2
            pl.when(along_x == 0)(functools.partial(write, keep_x, 0, total[:, :cut]))
            pl.when(along_x == 1)(functools.partial(write, send_x, 0, total[:, :cut]))
            pl.when(along_y == 0)(functools.partial(write, keep_y, 0, total[:, cut:]))
            pl.when(along_y == 1)(functools.partial(write, send_y, 0, total[:, cut:]))
        else:
            left = step < pl.num_programs(0) // 2
            pl.when(left)(functools.partial(write, (keep_x, send_x)[j % 2], j // 2, total))
            pl.when(~left)(functools.partial(write, (keep_y, send_y)[j // 2], j % 2, total))


def grad_call(a, b, order, got, tile, name):
    rows, cols = b.shape
    block = a.shape[1] // 8
    wide = block == 512
    steps = 4 if wide else cols // tile
    if wide:
        a_specs = [pl.BlockSpec((rows, block), lambda i, order: (0, order[i]))]
        b_spec = pl.BlockSpec((rows, cols), lambda i, order: (0, 0))
        full = pl.BlockSpec((1, block, cols), lambda i, order: (i, 0, 0))
        part = (1, block, cols // 2)
        maps = [lambda i, order: (i // 2, 0, 0), lambda i, order: (i // 2, 0, 0),
                lambda i, order: (jnp.minimum(i, 1), 0, 0), lambda i, order: (jnp.maximum(i - 2, 0), 0, 0)]
    else:
        a_specs = [pl.BlockSpec((rows, block), lambda i, order, j=j: (0, order[j])) for j in range(4)]
        b_spec = pl.BlockSpec((rows, tile), lambda i, order: (0, i))
        full = pl.BlockSpec((4, block, tile), lambda i, order: (0, 0, i))
        part = (2, block, tile)
        half = steps // 2
        maps = [lambda i, order: (0, 0, jnp.minimum(i, half - 1))] * 2
        maps += [lambda i, order: (0, 0, jnp.maximum(i - half, 0))] * 2
    if got is None:
        kernel, extra, extra_specs = grad_send_kernel, (), []
        out_specs, out_shape = full, jax.ShapeDtypeStruct((4, block, cols), jnp.float32)
    else:
        kernel, extra, extra_specs = functools.partial(grad_keep_kernel, wide=wide), (got,), [full]
        out_specs = [pl.BlockSpec(part, m) for m in maps]
        out_shape = [jax.ShapeDtypeStruct((2, block, cols // 2), jnp.float32)] * 4
    return pl.pallas_call(
        kernel,
        grid_spec=pltpu.PrefetchScalarGridSpec(num_scalar_prefetch=1, grid=(steps,),
                                               in_specs=a_specs + [b_spec] + extra_specs, out_specs=out_specs),
        out_shape=out_shape,
        cost_estimate=pl.CostEstimate(flops=8 * rows * block * cols, bytes_accessed=30_000_000, transcendentals=0),
        compiler_params=pltpu.CompilerParams(vmem_limit_bytes=60 * 1024 * 1024),
        name=name,
    )(order, *([a] * len(a_specs)), b, *extra)


class Reduction:
    def __init__(self, a, b, tile, name):
        self.a, self.b, self.tile, self.name = a, b, tile, name
        index = lax.axis_index("fsdp")
        self.blocks = jnp.stack([index, index ^ 2, index ^ 4, index ^ 6]).astype(jnp.int32)

    def begin(self, value):
        send = grad_call(self.a, self.b, self.blocks ^ 1, None, self.tile, self.name + "_send")
        value, send = lax.optimization_barrier((value, send))
        self.got = swap(send, 1)
        return value

    def sums(self):
        if self.got is not None:
            keep_x, send_x, keep_y, send_y = grad_call(self.a, self.b, self.blocks, self.got, self.tile, self.name)
            return [(keep_x, send_x), (keep_y, send_y)]
        if self.parts[0][0].ndim == 3:
            return [(keep[0] + got[0], keep[1] + got[1]) for keep, got in self.parts]
        return [(keep + got,) * 2 for keep, got in self.parts]

    def send(self, pairs):
        if self.got is not None:
            masks, self.got = (2, 4), None
        elif self.parts[0][0].ndim == 3:
            masks = (4, 2)
        else:
            masks = (8, 8)
        self.parts = [(keep, swap(out, mask)) for (keep, out), mask in zip(pairs, masks)]

    def result(self):
        return jnp.concatenate([keep + got for keep, got in self.parts], axis=1)


def advance(value, *reductions):
    value, pairs = lax.optimization_barrier((value, [r.sums() for r in reductions]))
    for reduction, pair in zip(reductions, pairs):
        reduction.send(pair)
    return value


def total_small(rows):
    index = lax.axis_index("fsdp")
    value = rows.reshape((2, 2, 2) + rows.shape[1:])
    for mask, mine, axis in ((1, index % 2, 2), (2, (index // 2) % 2, 1), (4, index // 4, 0)):
        value = pick(value, mine, axis) + swap(pick(value, 1 - mine, axis), mask)
    return value + swap(value, 8)


def layer_norm(t):
    mean = jnp.mean(t, axis=-1, keepdims=True)
    centered = t - mean
    rstd = lax.rsqrt(jnp.mean(centered * centered, axis=-1, keepdims=True) + LN_EPS)
    return centered * rstd, rstd


def layer_norm_back(grad, xhat, rstd):
    return rstd * (grad - jnp.mean(grad, axis=-1, keepdims=True) - xhat * jnp.mean(grad * xhat, axis=-1, keepdims=True))


ROWS = 400


def row_kernel(kernel, ins, weights, outs, sums, name, flops):
    tiles = ins[0].shape[0] // ROWS
    tile = lambda cols: pl.BlockSpec((ROWS, cols), lambda i: (i, 0))
    whole = lambda shape: pl.BlockSpec(shape, lambda i: (0,) * len(shape))
    in_specs = [tile(t.shape[1]) for t in ins] + [whole(t.shape) for t in weights]
    out_specs = [tile(cols) if isinstance(cols, int) else pl.BlockSpec((2,) + cols[1:], lambda i: (i, 0, 0))
                 for cols, _ in outs] + [whole((8, cols)) for cols in sums]
    out_shape = [jax.ShapeDtypeStruct((tiles * ROWS, cols) if isinstance(cols, int) else cols, dtype)
                 for cols, dtype in outs] + [jax.ShapeDtypeStruct((8, cols), jnp.float32) for cols in sums]

    def body(*refs):
        if sums:
            @pl.when(pl.program_id(0) == 0)
            def _():
                for ref in refs[len(refs) - len(sums):]:
                    ref[...] = jnp.zeros_like(ref)

        kernel(*refs)

    return pl.pallas_call(
        body, grid=(tiles,), in_specs=in_specs, out_specs=out_specs, out_shape=out_shape, name=name,
        cost_estimate=pl.CostEstimate(flops=flops, bytes_accessed=40_000_000, transcendentals=0),
        compiler_params=pltpu.CompilerParams(vmem_limit_bytes=60 * 1024 * 1024),
    )(*ins, *weights)


def total(t):
    return jnp.sum(t, axis=0, keepdims=True)


def out_kernel(o_ref, x_ref, w_ref, vec_ref, a_ref, y_ref, h_ref):
    for half in range(2):
        at = pl.ds(half * PAD, PAD)
        a = dot(o_ref[...][half * PAD:(half + 1) * PAD], w_ref[...]) + vec_ref[2:3]
        y = x_ref[...].astype(jnp.float32)[half * PAD:(half + 1) * PAD] + vec_ref[3:4] * a
        a_ref[at] = a
        y_ref[at] = y
        h_ref[at] = (layer_norm(y)[0] * vec_ref[4:5] + vec_ref[5:6]).astype(jnp.bfloat16)


def du_kernel(dm_ref, dact_ref, w_ref, du_ref, sum_ref):
    dm = dm_ref[...]
    for i in range(4):
        cols = slice(i * 1024, (i + 1) * 1024)
        du = dot(dm, w_ref[cols], ((1,), (1,))) * dact_ref[:, cols]
        du_ref[:, cols] = du.astype(jnp.bfloat16)
        sum_ref[0:1, cols] += total(du)


def dh2_kernel(du_ref, y_ref, dz_ref, a_ref, w_ref, vec_ref, dy_ref, da_ref, sum_ref):
    dh = dot(du_ref[...], w_ref[...], ((1,), (1,)))
    xhat, rstd = layer_norm(y_ref[...])
    sum_ref[0:1] += total(dh * xhat)
    sum_ref[1:2] += total(dh)
    dy = dz_ref[...].astype(jnp.float32) + layer_norm_back(dh * vec_ref[4:5], xhat, rstd)
    sum_ref[2:3] += total(dy * a_ref[...])
    da = dy * vec_ref[3:4]
    sum_ref[3:4] += total(da)
    dy_ref[...] = dy
    da_ref[...] = da.astype(jnp.bfloat16)


def dh1_kernel(tokens, first_ref, second_ref, x_ref, dy_ref, w_ref, vec_ref, dx_ref, sum_ref):
    dh = dot(first_ref[...], w_ref[:, :1536], ((1,), (1,))) + dot(second_ref[...], w_ref[:, 1536:], ((1,), (1,)))
    xhat, rstd = layer_norm(x_ref[...].astype(jnp.float32))
    sum_ref[0:1] += total(dh * xhat)
    sum_ref[1:2] += total(dh)
    dx = dy_ref[...] + layer_norm_back(dh * vec_ref[0:1], xhat, rstd)
    dx_ref[0] = dx[:tokens].astype(jnp.bfloat16)
    dx_ref[1] = dx[PAD:PAD + tokens].astype(jnp.bfloat16)


def gelu_parts(u):
    cdf = 0.5 + 0.5 * lax.erf(u * (0.5 ** 0.5))
    pdf = jnp.exp(-0.5 * u * u) * 0.3989422804014327
    return u * cdf, cdf + u * pdf


def dot(a, b, dims=((1,), (0,))):
    return lax.dot_general(a, b, (dims, ((), ())), preferred_element_type=jnp.float32)


def split_pair(block):
    wide = block.astype(jnp.float32)
    first = lax.broadcasted_iota(jnp.int32, wide.shape, 1) < 64
    return jnp.concatenate([jnp.where(first, wide, 0.0), jnp.where(first, 0.0, wide)], axis=0).astype(jnp.bfloat16)


def join_pair(stack):
    first = lax.broadcasted_iota(jnp.int32, (PAD, 128), 1) < 64
    return jnp.where(first, stack[:PAD], stack[PAD:])


def masked_scores(q2, k, tokens):
    scores = dot(q2, k, ((1,), (1,)))
    keys = lax.broadcasted_iota(jnp.int32, scores.shape, 1)
    return jnp.where(keys < tokens, scores * 0.125, -1e30)


def attend_kernel(tokens, qkv_ref, o_ref, lse_ref):
    lanes = lax.broadcasted_iota(jnp.int32, (PAD, 128), 1)
    stats = jnp.zeros((PAD, 128), jnp.float32)
    for pair in range(8):
        at = (pair // 4) * 1536 + (pair % 4) * 128
        q, k, v = (qkv_ref[0, :, at + 512 * i:at + 512 * i + 128] for i in range(3))
        scores = masked_scores(split_pair(q), k, tokens)
        top = jnp.max(scores, axis=1, keepdims=True)
        exps = jnp.exp(scores - top)
        total = jnp.sum(exps, axis=1, keepdims=True)
        probs = (exps * (1.0 / total)).astype(jnp.bfloat16)
        o_ref[0, :, pair * 128:(pair + 1) * 128] = join_pair(dot(probs, v)).astype(jnp.bfloat16)
        lse = top + jnp.log(total)
        stats = jnp.where(lanes == 2 * pair, lse[:PAD], stats)
        stats = jnp.where(lanes == 2 * pair + 1, lse[PAD:], stats)
    lse_ref[0] = stats


def attend(qkv, tokens):
    seqs = qkv.shape[0]
    return pl.pallas_call(
        functools.partial(attend_kernel, tokens),
        grid=(seqs,),
        in_specs=[pl.BlockSpec((1, PAD, 3072), lambda s: (s, 0, 0))],
        out_specs=[pl.BlockSpec((1, PAD, 1024), lambda s: (s, 0, 0)), pl.BlockSpec((1, PAD, 128), lambda s: (s, 0, 0))],
        out_shape=[jax.ShapeDtypeStruct((seqs, PAD, 1024), jnp.bfloat16),
                   jax.ShapeDtypeStruct((seqs, PAD, 128), jnp.float32)],
        cost_estimate=pl.CostEstimate(flops=20_000_000_000, bytes_accessed=20_000_000, transcendentals=8_000_000),
        name="attend",
    )(qkv)


def attend_back_kernel(tokens, base, qkv_ref, do_ref, lse_ref, dqkv_ref, db_ref):
    @pl.when(pl.program_id(0) == 0)
    def _():
        db_ref[...] = jnp.zeros_like(db_ref)

    for pair in range(4):
        cols = [slice(512 * i + pair * 128, 512 * i + (pair + 1) * 128) for i in range(3)]
        q2, k, v = split_pair(qkv_ref[0, :, cols[0]]), qkv_ref[0, :, cols[1]], qkv_ref[0, :, cols[2]]
        do2 = split_pair(do_ref[0, :, cols[0]])
        head = base + 2 * pair
        lse = jnp.concatenate([lse_ref[0, :, head:head + 1], lse_ref[0, :, head + 1:head + 2]], axis=0)
        probs = jnp.exp(masked_scores(q2, k, tokens) - lse)
        dprobs = dot(do2, v, ((1,), (1,)))
        delta = jnp.sum(dprobs * probs, axis=1, keepdims=True)
        dscores = (probs * (dprobs - delta) * 0.125).astype(jnp.bfloat16)
        dv = dot(probs.astype(jnp.bfloat16), do2, ((0,), (0,)))
        dk = dot(dscores, q2, ((0,), (0,)))
        dq = join_pair(dot(dscores, k))
        for col, value in zip(cols, (dq, dk, dv)):
            dqkv_ref[0, :, col] = value.astype(jnp.bfloat16)
            db_ref[0:1, col] += jnp.sum(value, axis=0, keepdims=True)


def attend_back(qkv, do, lse, tokens, part):
    seqs = qkv.shape[0]
    return pl.pallas_call(
        functools.partial(attend_back_kernel, tokens, part * 8),
        grid=(seqs,),
        in_specs=[pl.BlockSpec((1, PAD, 1536), lambda s: (s, 0, part)), pl.BlockSpec((1, PAD, 512), lambda s: (s, 0, part)),
                  pl.BlockSpec((1, PAD, 128), lambda s: (s, 0, 0))],
        out_specs=[pl.BlockSpec((1, PAD, 1536), lambda s: (s, 0, 0)), pl.BlockSpec((8, 1536), lambda s: (0, 0))],
        out_shape=[jax.ShapeDtypeStruct((seqs, PAD, 1536), jnp.bfloat16), jax.ShapeDtypeStruct((8, 1536), jnp.float32)],
        cost_estimate=pl.CostEstimate(flops=25_000_000_000, bytes_accessed=15_000_000, transcendentals=4_000_000),
        name=f"attend_back_{part}",
    )(qkv, do, lse)


def by_part(t):
    return t.reshape(t.shape[:-1] + (3, 2, 512)).swapaxes(-3, -2).reshape(t.shape)


def gather_params(shards):
    w_qkv, b_qkv, w_out, w_up, b_up, w_down, vec_params = shards

    def full_rows(shard):
        return lax.all_gather(shard.astype(jnp.bfloat16), "fsdp", axis=0, tiled=True)

    small = jnp.concatenate([vec_params, b_qkv.reshape(3, 128), b_up.reshape(4, 128)], axis=0).astype(jnp.bfloat16)
    small = lax.all_gather(small, "fsdp", axis=0).astype(jnp.float32)
    vec = small[:, :8].transpose(1, 0, 2).reshape(8, 1024)
    return (full_rows(by_part(w_qkv)), by_part(small[:, 8:11].reshape(3072)), full_rows(w_out), full_rows(w_up),
            small[:, 11:15].reshape(4096), full_rows(w_down), vec)


def device_step(x_loc, dz_loc, *shards):
    w_qkv, b_qkv, w_out, w_up, b_up, w_down, vec = gather_params(shards)
    g1, c1, bo, s1, g2, c2, b2, s2 = vec
    seqs, tokens, width = x_loc.shape
    rows = seqs * PAD
    pad = ((0, 0), (0, PAD - tokens), (0, 0))
    x_bf, dz_bf = jnp.pad(x_loc, pad).reshape(rows, width), jnp.pad(dz_loc, pad).reshape(rows, width)
    x, dz = x_bf.astype(jnp.float32), dz_bf.astype(jnp.float32)
    bf = lambda t: t.astype(jnp.bfloat16)

    xhat1, rstd1 = layer_norm(x)
    h1 = bf(xhat1 * g1 + c1)
    qkv = bf(dot(h1, w_qkv) + b_qkv).reshape(seqs, PAD, 3 * width)
    o, lse = attend(qkv, tokens)
    o = o.reshape(rows, width)
    bf16, f32 = jnp.bfloat16, jnp.float32
    a, y, h2 = row_kernel(out_kernel, (o, x_bf), (w_out, vec), ((width, f32), (width, f32), (width, bf16)), (),
                          "out", 5_000_000_000)
    u = dot(h2, w_up) + b_up
    act, dact = gelu_parts(u)
    act = bf(act)

    dm = dz * s2
    dm_bf = bf(dm)
    down = Reduction(act, dm_bf, 1024, "grad_down")
    dm_bf, act = down.begin((dm_bf, act))
    du_bf, sum_up = row_kernel(du_kernel, (dm_bf, dact), (w_down,), ((4 * width, bf16),), (4 * width,), "du", 20_000_000_000)
    du_bf = advance(du_bf, down)
    up = Reduction(h2, du_bf, 1024, "grad_up")
    du_bf = up.begin(du_bf)
    dy, da_bf, sum_mid = row_kernel(dh2_kernel, (du_bf, y, dz_bf, a), (w_up, vec), ((width, f32), (width, bf16)), (width,),
                                    "dh2", 20_000_000_000)
    da_bf = advance(da_bf, down, up)
    out = Reduction(o, da_bf, 512, "grad_out")
    da_bf = out.begin(da_bf)
    do = bf(dot(da_bf, w_out, ((1,), (1,)))).reshape(seqs, PAD, width)
    do = advance(do, down)
    dqkv0, db0 = attend_back(qkv, do, lse, tokens, 0)
    dqkv0, do = advance((dqkv0.reshape(rows, 1536), do), up, out)
    first = Reduction(h1, dqkv0, 768, "grad_qkv0")
    do = first.begin(do)
    dqkv1, db1 = attend_back(qkv, do, lse, tokens, 1)
    dqkv1 = advance(dqkv1.reshape(rows, 1536), up, out, first)
    second = Reduction(h1, dqkv1, 768, "grad_qkv1")
    dqkv1, act = second.begin((dqkv1, act))
    m = dot(act, w_down) + b2
    z = bf(y + s2 * m)
    grad_s2 = jnp.sum(dz * m, axis=0)
    grad_b2 = jnp.sum(dm, axis=0)
    z, dqkv1 = advance((z, dqkv1), out, first, second)
    dx, sum_last = row_kernel(functools.partial(dh1_kernel, tokens), (dqkv0, dqkv1, x_bf, dy), (w_qkv, vec),
                              ((x_loc.shape, bf16),), (width,), "dh1", 15_000_000_000)
    grad_b_qkv = jnp.concatenate([db0[0].reshape(3, 1, 512), db1[0].reshape(3, 1, 512)], axis=1)
    grad_vec = jnp.stack([sum_last[0], sum_last[1], sum_mid[3], sum_mid[2], sum_mid[0], sum_mid[1], grad_b2, grad_s2])
    small = jnp.concatenate([grad_vec.reshape(8, 8, 128).transpose(1, 0, 2), grad_b_qkv.reshape(8, 3, 128),
                             sum_up[0].reshape(8, 4, 128)], axis=1)
    small, dx = advance((small, dx), first, second)
    small = total_small(small)
    small, dx = advance((small, dx), second)
    grad_w_qkv = jnp.concatenate([r.result().reshape(128, 3, 1, 512) for r in (first, second)], axis=2)
    grad_w_qkv = grad_w_qkv.reshape(128, 3072)
    grad_w_out, grad_w_up, grad_w_down = out.result(), up.result(), down.result()
    unpad = lambda t: t.reshape(seqs, PAD, width)[:, :tokens]
    return (unpad(z), dx, grad_w_qkv, small[8:11].reshape(384), grad_w_out, grad_w_up,
            small[11:15].reshape(512), grad_w_down, small[:8])


def solution(mesh):
    batch = P(("rep", "fsdp"), None, None)
    row, flat, col = P("fsdp", None), P("fsdp"), P(None, "fsdp")
    params = (row, flat, row, row, flat, row, col)
    return jax.shard_map(device_step, mesh=mesh, in_specs=(batch, batch) + params,
                         out_specs=(batch, batch) + params, check_vma=False)
```
